32 devices in a mesh: dp: 8 (over z, y), tensor: 4 (over x, core).
Axes of the slice: x: 2, y: 2, z: 4, core: 2. Of those that a mesh axis runs over, the one named last changes fastest.
Arguments:
- sampled_earlier_tokens: int32 [32, 169], P('dp'), may hold values from 0 to 4095
- quantizer_vectors: float32 [4096, 32], replicated, may hold values from -6 to 6
- summed_latent_canvas: float32 [32, 256, 32], P('dp'), may hold values from -6 to 6
- latent_lift_matrix: float32 [32, 1536], replicated, may hold values from -1 to 1
- location_tier_offset: float32 [256, 1536], replicated, may hold values from -3 to 3
- adaptive_norm_factors: float32 [1, 32, 6, 1536], P(None, 'dp'), may hold values from -3 to 3
- logit_sharpness: float32 [1, 16], P(None, 'tensor'), may hold values from 2 to 240, as said below
- probe_match_content_matrix: bfloat16 [1, 1536, 3, 1536], P(None, 'dp', None, 'tensor'), may hold values from -1 to 1, as said below
- mixing_projection_matrix: bfloat16 [1, 1536, 1536], P(None, 'tensor', 'dp'), may hold values from -0.15625 to 0.15625
- widening_projection_matrix: bfloat16 [1, 1536, 6144], P(None, 'dp', 'tensor'), may hold values from -0.15625 to 0.15625
- narrowing_projection_matrix: bfloat16 [1, 6144, 1536], P(None, 'tensor', 'dp'), may hold values from -0.078125 to 0.078125
- cached_lower_grid_lookups: bfloat16 [1, 32, 424, 1536], P(None, 'dp', None, 'tensor'), may hold values from -6 to 6
- cached_lower_grid_payloads: bfloat16 [1, 32, 424, 1536], P(None, 'dp', None, 'tensor'), may hold values from -6 to 6
- final_norm_factors: float32 [32, 2, 1536], P('dp'), may hold values from -3 to 3
- vocabulary_logit_matrix: bfloat16 [1536, 4096], P(None, 'tensor'), may hold values from -0.15625 to 0.15625
Outputs:
- logits: bfloat16 [32, 256, 4096], P('dp', None, 'tensor')
- canvas: float32 [32, 256, 32], P('dp')
The draws below stay inside these ranges and needn't reach their ends.
Inputs may be any that keep to these rules, and one draw needn't show every extreme that they name: `logit_sharpness`: Positive. `probe_match_content_matrix`: entries of spread about 1536 ** -0.5.
All inputs are finite; a program needn't handle non-finite values.
Results may differ from the reference program's by a relative error of at most 0.015.
Values may be sent and summed in bfloat16 or wider, within the bound.
No kernel may reach another device: no remote copies, remote signals or barrier semaphores. Data moves between devices by JAX's collectives and lax.ppermute only.
A program may use at most 128 MiB of HBM per device.

```python
import math
import jax
import jax.numpy as jnp
from jax import lax

D = 1536
HEADS = 16
HDIM = 96
FF = 6144
VOCAB = 4096
CVAE = 32
LAYERS = 1
SIDE = 16
PREV = 13
CACHE = 424
TOK = 256
PREVTOK = 169
IMAGES = 32
N_TENSOR = 4


def draw_probe_match_content_matrix(key, part):
    base_draw = jax.random.truncated_normal(jax.random.fold_in(key, 11), -6.0, 6.0, (LAYERS, D, 3, D), jnp.float32) * D ** (-0.5)
    drawn_values = base_draw
    return drawn_values.astype(jnp.bfloat16)


def draw_logit_sharpness(key, part):
    exponent = jax.random.uniform(jax.random.fold_in(key, 23), (LAYERS, HEADS), jnp.float32, math.log(2.0), math.log(60.0))
    drawn_values = jnp.exp(exponent)
    return drawn_values


def plant(array, stream_key, least, top_value):
    extent = array.shape
    place = [jax.random.randint(jax.random.fold_in(stream_key, axis), (), 0, extent[axis]) for axis in range(len(extent))]
    array = array.at[tuple(place)].set(least)
    longest = extent.index(max(extent))
    place[longest] = (place[longest] + 1) % extent[longest]
    return array.at[tuple(place)].set(top_value)


def block_levels(key, dims, pieces, smallest, largest):
    factor_of = 1.0
    for dim, parts in pieces:
        draws = jax.random.uniform(jax.random.fold_in(jax.random.fold_in(key, 6), dim), (parts,), jnp.float32, smallest / len(pieces), largest / len(pieces))
        factor_of = factor_of * jnp.repeat(jnp.exp(draws), dims[dim] // parts).reshape((-1,) + (1,) * (len(dims) - 1 - dim))
    return factor_of


def noise(key, dims, width, bound, cuts=(), kind=jnp.bfloat16):
    array = jax.random.normal(key, dims, jnp.float32) * width
    if len(cuts) > 0:
        array = block_levels(key, dims, cuts, -0.22, 0.18) * array
    return jnp.clip(array, min=-bound, max=bound).astype(kind)


def setup_inputs(seed: int = 0) -> dict:
    streams_of = jax.random.split(jax.random.key(seed), 16)
    return {
        "sampled_earlier_tokens": plant(jax.random.randint(streams_of[0], (IMAGES, PREVTOK), 0, VOCAB), jax.random.fold_in(streams_of[0], 1), 0, VOCAB - 1).astype(jnp.int32),
        "quantizer_vectors": noise(streams_of[1], (VOCAB, CVAE), 1.0, 6.0, (), jnp.float32),
        "summed_latent_canvas": noise(streams_of[2], (IMAGES, TOK, CVAE), 1.0, 6.0, ((0, 8),), jnp.float32),
        "latent_lift_matrix": noise(streams_of[3], (CVAE, D), CVAE ** -0.5, 1.0, (), jnp.float32),
        "location_tier_offset": noise(streams_of[4], (TOK, D), 0.5, 3.0, (), jnp.float32),
        "adaptive_norm_factors": noise(streams_of[5], (LAYERS, IMAGES, 6, D), 0.5, 3.0, ((1, 8),), jnp.float32),
        "logit_sharpness": draw_logit_sharpness(jax.random.fold_in(streams_of[15], 71), 0),
        "probe_match_content_matrix": draw_probe_match_content_matrix(jax.random.fold_in(streams_of[15], 71), 0),
        "mixing_projection_matrix": noise(streams_of[8], (LAYERS, D, D), D ** -0.5, 0.15625, ((1, 4), (2, 8))),
        "widening_projection_matrix": noise(streams_of[9], (LAYERS, D, FF), D ** -0.5, 0.15625, ((1, 8), (2, 4))),
        "narrowing_projection_matrix": noise(streams_of[10], (LAYERS, FF, D), FF ** -0.5, 0.078125, ((1, 4), (2, 8))),
        "cached_lower_grid_lookups": noise(streams_of[11], (LAYERS, IMAGES, CACHE, D), 1.0, 6.0, ((1, 8), (3, 4))),
        "cached_lower_grid_payloads": noise(streams_of[12], (LAYERS, IMAGES, CACHE, D), 1.0, 6.0, ((1, 8), (3, 4))),
        "final_norm_factors": noise(streams_of[13], (IMAGES, 2, D), 0.5, 3.0, ((0, 8),), jnp.float32),
        "vocabulary_logit_matrix": noise(streams_of[14], (D, VOCAB), D ** -0.5, 0.15625, ((1, 4),)),
    }


norm_floor = 0.1
highest = lax.Precision.HIGHEST

def interp_matrix(grid_side, prev_side):
    out_cells = jnp.arange(grid_side, dtype=jnp.int32)
    numerator = jnp.maximum((2 * out_cells + 1) * prev_side - grid_side, 0)
    lower_cell = numerator // (2 * grid_side)
    fraction = (numerator % (2 * grid_side)).astype(jnp.float32) / (2.0 * grid_side)
    upper_cell = jnp.minimum(lower_cell + 1, prev_side - 1)
    in_cells = jnp.arange(prev_side, dtype=jnp.int32)
    lower_hit = (in_cells[None, :] == lower_cell[:, None]).astype(jnp.float32)
    upper_hit = (in_cells[None, :] == upper_cell[:, None]).astype(jnp.float32)
    return lower_hit * (1.0 - fraction)[:, None] + upper_hit * fraction[:, None]

def modulate(stream, scale_vec, shift_vec):
    center = stream - lax.optimization_barrier(jnp.mean(stream, axis=-1, keepdims=True))
    variance = lax.optimization_barrier(jnp.mean(center * center, axis=-1, keepdims=True))
    return center * lax.rsqrt(variance + norm_floor) * (1.0 + scale_vec) + shift_vec

def hidden_neuron_slice(vectors):
    return vectors * lax.rsqrt(lax.optimization_barrier(jnp.sum(vectors * vectors, axis=-1, keepdims=True)) + 1.0)

def group_sum(left_rows, weight, groups):
    part_width = left_rows.shape[1] // groups
    running = jnp.zeros((left_rows.shape[0], weight.shape[1]), jnp.float32)
    for group_id in range(groups):
        partial_value = jnp.dot(left_rows[:, group_id * part_width:(group_id + 1) * part_width], weight[group_id * part_width:(group_id + 1) * part_width], preferred_element_type=jnp.float32)
        rounded = lax.optimization_barrier(partial_value.astype(jnp.bfloat16))
        running = running + rounded.astype(jnp.float32)
    return running

def attend_image(operands):
    probe_token_slab, keys_all, values_all = operands
    scores = jnp.einsum('thd,shd->hts', probe_token_slab.astype(jnp.float32), keys_all.astype(jnp.float32), precision=highest)
    row_max = lax.optimization_barrier(jnp.max(scores, axis=-1, keepdims=True))
    shifted = jnp.exp(scores - row_max)
    weights_bf = (shifted / lax.optimization_barrier(jnp.sum(shifted, axis=-1, keepdims=True))).astype(jnp.bfloat16)
    attended = jnp.einsum('hts,shd->thd', weights_bf.astype(jnp.float32), values_all.astype(jnp.float32), precision=highest)
    return attended.astype(jnp.bfloat16)

def reference(sampled_earlier_tokens, quantizer_vectors, summed_latent_canvas, latent_lift_matrix, location_tier_offset, adaptive_norm_factors, logit_sharpness, probe_match_content_matrix, mixing_projection_matrix, widening_projection_matrix, narrowing_projection_matrix, cached_lower_grid_lookups, cached_lower_grid_payloads, final_norm_factors, vocabulary_logit_matrix):
    vocab_ids = jnp.arange(VOCAB, dtype=jnp.int32)

    def embed_image(token_ids):
        onehot = (token_ids[:, None] == vocab_ids[None, :]).astype(jnp.float32)
        return jnp.dot(onehot, quantizer_vectors, precision=highest, preferred_element_type=jnp.float32)
    embedded = lax.map(embed_image, sampled_earlier_tokens).reshape(IMAGES, PREV, PREV, CVAE)
    up_matrix = interp_matrix(SIDE, PREV)
    lifted = jnp.einsum('ai,nijc->najc', up_matrix, embedded, precision=highest)
    lifted = jnp.einsum('bj,najc->nabc', up_matrix, lifted, precision=highest)
    canvas = summed_latent_canvas + lifted.reshape(IMAGES, TOK, CVAE)
    stream = jnp.einsum('ntc,cd->ntd', canvas, latent_lift_matrix, precision=highest) + location_tier_offset[None]
    for depth_ordinal in range(LAYERS):
        factors = adaptive_norm_factors[depth_ordinal]
        normed = modulate(stream, factors[:, 2][:, None], factors[:, 4][:, None]).astype(jnp.bfloat16)
        projected = jnp.dot(normed.reshape(IMAGES * TOK, D), probe_match_content_matrix[depth_ordinal].reshape(D, 3 * D), preferred_element_type=jnp.float32)
        complete_channel_group_set = projected.reshape(IMAGES, TOK, 3, HEADS, HDIM)
        probe_token_slab = (hidden_neuron_slice(complete_channel_group_set[:, :, 0]) * logit_sharpness[depth_ordinal][None, None, :, None]).astype(jnp.bfloat16)
        key_new = hidden_neuron_slice(complete_channel_group_set[:, :, 1]).astype(jnp.bfloat16)
        value_new = complete_channel_group_set[:, :, 2].astype(jnp.bfloat16)
        key_old = hidden_neuron_slice(cached_lower_grid_lookups[depth_ordinal].astype(jnp.float32).reshape(IMAGES, CACHE, HEADS, HDIM)).astype(jnp.bfloat16)
        value_old = cached_lower_grid_payloads[depth_ordinal].reshape(IMAGES, CACHE, HEADS, HDIM)
        keys_all = jnp.concatenate([key_old, key_new], axis=1)
        values_all = jnp.concatenate([value_old, value_new], axis=1)
        attended = lax.map(attend_image, (probe_token_slab, keys_all, values_all))
        mixed_rows = group_sum(attended.reshape(IMAGES * TOK, D), mixing_projection_matrix[depth_ordinal], N_TENSOR)
        stream = stream + factors[:, 0][:, None] * mixed_rows.reshape(IMAGES, TOK, D)
        normed = modulate(stream, factors[:, 3][:, None], factors[:, 5][:, None]).astype(jnp.bfloat16)
        hidden = jax.nn.gelu(jnp.dot(normed.reshape(IMAGES * TOK, D), widening_projection_matrix[depth_ordinal], preferred_element_type=jnp.float32), approximate=True).astype(jnp.bfloat16)
        mixed_rows = group_sum(hidden, narrowing_projection_matrix[depth_ordinal], N_TENSOR)
        stream = stream + factors[:, 1][:, None] * mixed_rows.reshape(IMAGES, TOK, D)
    normed = modulate(stream, final_norm_factors[:, 0][:, None], final_norm_factors[:, 1][:, None]).astype(jnp.bfloat16)
    logits = jnp.dot(normed.reshape(IMAGES * TOK, D), vocabulary_logit_matrix, preferred_element_type=jnp.float32).astype(jnp.bfloat16)
    return (logits.reshape(IMAGES, TOK, VOCAB), canvas)
```

```python
import functools
import math

import jax
import jax.numpy as jnp
import numpy as np
from jax import lax
from jax.experimental import pallas as pl
from jax.experimental.pallas import tpu as pltpu
from jax.sharding import PartitionSpec as P


norm_floor = 0.1
highest = lax.Precision.HIGHEST
f32 = jnp.float32
bf16 = jnp.bfloat16
ANY = pl.BlockSpec(memory_space=pl.ANY)
SMEM = pl.BlockSpec(memory_space=pltpu.SMEM)
AXES = ("dp", "tensor")


def interp_matrix(grid_side, prev_side):
    out = np.zeros((grid_side, prev_side), np.float32)
    for a in range(grid_side):
        top = max((2 * a + 1) * prev_side - grid_side, 0)
        low = top // (2 * grid_side)
        frac = (top % (2 * grid_side)) / (2.0 * grid_side)
        out[a, low] += 1.0 - frac
        out[a, min(low + 1, prev_side - 1)] += frac
    return out


def whole(shape):
    return pl.BlockSpec(shape, lambda *_: (0,) * len(shape))


def params(mib):
    return pltpu.CompilerParams(vmem_limit_bytes=mib * 1024 * 1024)


def split3(x):
    hi = x.astype(bf16)
    rest = x - hi.astype(f32)
    mid = rest.astype(bf16)
    low = (rest - mid.astype(f32)).astype(bf16)
    return hi, mid, low


NT = (((1,), (1,)), ((), ()))


def canvas_body(tok_ref, book_ref, kron_ref, base_ref, out_ref):
    rows = book_ref.shape[0]
    entries = book_ref.shape[1]
    tok = tok_ref[0]
    ids = lax.broadcasted_iota(jnp.int32, (entries, tok.shape[1]), 0)
    onehot = jnp.where(ids == tok, 1.0, 0.0).astype(bf16)
    parts = jnp.concatenate(split3(book_ref[...]), axis=0)
    picked = jnp.dot(parts, onehot, preferred_element_type=f32)
    picked = picked[:rows] + picked[rows : 2 * rows] + picked[2 * rows :]
    lifted = lax.dot_general(
        kron_ref[...], picked, NT, precision=highest, preferred_element_type=f32
    )
    out_ref[0] = base_ref[0] + lifted


def canvas_call(tokens, book_t, kron, base):
    images, count = tokens.shape
    return pl.pallas_call(
        canvas_body,
        grid=(images,),
        in_specs=[
            pl.BlockSpec((1, 1, count), lambda i: (i, 0, 0)),
            whole(book_t.shape),
            whole(kron.shape),
            pl.BlockSpec((1,) + base.shape[1:], lambda i: (i, 0, 0)),
        ],
        out_specs=pl.BlockSpec((1,) + base.shape[1:], lambda i: (i, 0, 0)),
        out_shape=jax.ShapeDtypeStruct(base.shape, f32),
        compiler_params=params(24),
        name="canvas",
    )(tokens.reshape(images, 1, count), book_t, kron, base)


def modulate(stream, scale_vec, shift_vec):
    center = stream - jnp.mean(stream, axis=-1, keepdims=True)
    variance = jnp.mean(center * center, axis=-1, keepdims=True)
    return center * lax.rsqrt(variance + norm_floor) * (1.0 + scale_vec) + shift_vec


def enter_body(half_ref, canvas_ref, lift_ref, loc_ref, fac_ref, normed_ref, stream_ref):
    span = stream_ref.shape[0]
    own = half_ref[0]
    for k in range(2):
        start = pl.multiple_of((own if k == 0 else 1 - own) * span, span)
        stream = (
            jnp.dot(
                canvas_ref[0, pl.ds(start, span), :],
                lift_ref[...],
                precision=highest,
                preferred_element_type=f32,
            )
            + loc_ref[pl.ds(start, span), :]
        )
        if k == 0:
            stream_ref[...] = stream
        normed_ref[pl.ds(k * span, span), :] = modulate(
            stream, fac_ref[0, 2:3, :], fac_ref[0, 4:5, :]
        ).astype(bf16)


def enter_call(i, half, canvas, lift, loc, factors):
    tokens, width = loc.shape
    return pl.pallas_call(
        enter_body,
        grid=(1,),
        in_specs=[
            SMEM,
            pl.BlockSpec((1,) + canvas.shape[1:], lambda _: (i, 0, 0)),
            whole(lift.shape),
            whole(loc.shape),
            pl.BlockSpec((1,) + factors.shape[1:], lambda _: (i, 0, 0)),
        ],
        out_specs=[whole((tokens, width)), whole((tokens // 2, width))],
        out_shape=[
            jax.ShapeDtypeStruct((tokens, width), bf16),
            jax.ShapeDtypeStruct((tokens // 2, width), f32),
        ],
        compiler_params=params(24),
        name="enter",
    )(half, canvas, lift, loc, factors)


def head_windows(heads, size):
    total = heads * size
    spans = []
    for h in range(heads):
        low = (h * size) // 128 * 128
        high = min(-(-((h + 1) * size) // 128) * 128, total)
        spans.append((low, high))
    return spans


def head_scale(x, heads, size, extra):
    lane = lax.broadcasted_iota(jnp.int32, (1, x.shape[1]), 1)
    square = x * x
    scale = None
    for h, (low, high) in enumerate(head_windows(heads, size)):
        inside = (lane[:, low:high] >= h * size) & (lane[:, low:high] < (h + 1) * size)
        total = jnp.sum(jnp.where(inside, square[:, low:high], 0.0), axis=1, keepdims=True)
        factor = lax.rsqrt(total + 1.0)
        if extra is not None:
            factor = factor * extra(h)
        if scale is None:
            scale = jnp.broadcast_to(factor, x.shape)
        else:
            scale = jnp.where(lane >= h * size, factor, scale)
    return (x * scale).astype(bf16)


def attend_body(heads, size, count, *refs):
    place_ref, sharp_ref, normed_ref, oldk_ref, oldv_ref = refs[:5]
    chunks = refs[5 : 5 + count]
    keep_ref, send_ref, weight, sems = refs[5 + count :]
    width = heads * size
    copies = []
    for k, chunk in enumerate(chunks):
        start = pl.multiple_of(place_ref[k], 16)
        copy = pltpu.make_async_copy(
            chunk, weight.at[pl.ds(start, chunk.shape[0]), :], sems.at[k]
        )
        copy.start()
        copies.append(copy)
    key_old = head_scale(oldk_ref[0, 0].astype(f32), heads, size, None)
    value_old = oldv_ref[0, 0]
    for copy in copies:
        copy.wait()
    normed = normed_ref[...]
    part = [
        jnp.dot(normed, weight[:, k * width : (k + 1) * width], preferred_element_type=f32)
        for k in range(3)
    ]
    query = head_scale(part[0], heads, size, lambda h: sharp_ref[0, h])
    key_new = head_scale(part[1], heads, size, None)
    value_new = part[2].astype(bf16)
    lane = lax.broadcasted_iota(jnp.int32, (1, width), 1)
    rows = normed.shape[0]
    pieces = [jnp.zeros((rows, 128), f32) for _ in range(-(-width // 128))]
    for h, (low, high) in enumerate(head_windows(heads, size)):
        inside = (lane[:, low:high] >= h * size) & (lane[:, low:high] < (h + 1) * size)
        q = jnp.where(inside, query[:, low:high].astype(f32), 0.0).astype(bf16)
        s_old = lax.dot_general(q, key_old[:, low:high], NT, preferred_element_type=f32)
        s_new = lax.dot_general(q, key_new[:, low:high], NT, preferred_element_type=f32)
        top = jnp.maximum(
            jnp.max(s_old, axis=1, keepdims=True), jnp.max(s_new, axis=1, keepdims=True)
        )
        e_old = jnp.exp(s_old - top)
        e_new = jnp.exp(s_new - top)
        total = jnp.sum(e_old, axis=1, keepdims=True) + jnp.sum(e_new, axis=1, keepdims=True)
        out = jnp.dot(e_old.astype(bf16), value_old[:, low:high], preferred_element_type=f32)
        out = out + jnp.dot(
            e_new.astype(bf16), value_new[:, low:high], preferred_element_type=f32
        )
        out = jnp.where(inside, out * (1.0 / total), 0.0)
        for t in range(low // 128, -(-high // 128)):
            at = t * 128 - low
            pieces[t] = pieces[t] + out[:, at : at + 128]
    attended = jnp.concatenate(pieces, axis=1)[:, :width].astype(bf16)
    mixed = lax.dot_general(
        attended, weight[:, 3 * width :], NT, preferred_element_type=f32
    ).astype(bf16)
    keep_ref[...] = mixed[: rows // 2]
    send_ref[...] = mixed[rows // 2 :]


def attend_call(i, heads, size, sharp, place, normed, old_k, old_v, chunks):
    rows, width = normed.shape
    cache = pl.BlockSpec((1, 1) + old_k.shape[2:], lambda _: (0, i, 0, 0))
    out = jax.ShapeDtypeStruct((rows // 2, width), bf16)
    return pl.pallas_call(
        functools.partial(attend_body, heads, size, len(chunks)),
        grid=(1,),
        in_specs=[SMEM, SMEM, whole(normed.shape), cache, cache] + [ANY] * len(chunks),
        out_specs=[whole(out.shape)] * 2,
        out_shape=[out, out],
        scratch_shapes=[
            pltpu.VMEM((width, chunks[0].shape[1]), bf16),
            pltpu.SemaphoreType.DMA((len(chunks),)),
        ],
        compiler_params=params(32),
        name="attend",
    )(place, sharp, normed, old_k, old_v, *chunks)


def mid_body(stream_ref, near_ref, far_ref, fac_ref, *rest):
    out_ref, normed_ref = rest[-2:]
    mixed = near_ref[...].astype(f32) + far_ref[...].astype(f32)
    stream = stream_ref[...] + fac_ref[0, 0:1, :] * mixed
    out_ref[...] = stream
    normed_ref[...] = modulate(stream, fac_ref[0, 3:4, :], fac_ref[0, 5:6, :]).astype(bf16)


def mid_call(i, images, stream, near, far, factors, before):
    span, width = stream.shape
    steps = 2
    spec = pl.BlockSpec((span // steps, width), lambda k: (k, 0))
    extra = [] if before is None else [before]
    return pl.pallas_call(
        mid_body,
        grid=(steps,),
        in_specs=[
            spec,
            spec,
            spec,
            pl.BlockSpec((1,) + factors.shape[1:], lambda _: (i, 0, 0)),
        ]
        + [ANY] * len(extra),
        out_specs=[
            pl.BlockSpec((span // steps, width), lambda k: (i * steps + k, 0)),
            spec,
        ],
        out_shape=[
            jax.ShapeDtypeStruct((images * span, width), f32),
            jax.ShapeDtypeStruct(stream.shape, bf16),
        ],
        input_output_aliases={4: 0} if extra else {},
        compiler_params=params(16),
        name="mid",
    )(stream, near, far, factors, *extra)


def widen_body(pieces, count, *refs):
    place_ref = refs[0]
    rows_refs = refs[1 : 1 + pieces]
    chunks = refs[1 + pieces : 1 + pieces + count]
    outs = refs[1 + pieces + count : 3 + pieces + count]
    source, weight, sems = refs[3 + pieces + count :]
    span = rows_refs[0].shape[0]
    copies = []
    for k, chunk in enumerate(chunks):
        start = pl.multiple_of(place_ref[k], 16)
        copies.append(
            pltpu.make_async_copy(
                chunk, weight.at[pl.ds(start, chunk.shape[0]), :], sems.at[k]
            )
        )
    for k, piece in enumerate(rows_refs):
        copies.append(
            pltpu.make_async_copy(
                piece, source.at[k * span : (k + 1) * span, :], sems.at[count + k]
            )
        )
    for copy in copies:
        copy.start()
    for copy in copies:
        copy.wait()
    step = 512 if weight.shape[1] % 512 == 0 else weight.shape[1]
    half = source.shape[0] // 2
    for low in range(0, weight.shape[1], step):
        for k in range(2):
            u = jnp.dot(
                source[k * half : (k + 1) * half, :],
                weight[:, low : low + step],
                preferred_element_type=f32,
            )
            outs[k][:, low : low + step] = (
                0.5 * u * (1.0 + jnp.tanh(math.sqrt(2.0 / math.pi) * (u + 0.044715 * (u * u * u))))
            ).astype(bf16)


def widen_call(place, rows, chunks):
    span, width = rows[0].shape
    shape = (span * len(rows) // 2, chunks[0].shape[1])
    out = jax.ShapeDtypeStruct(shape, bf16)
    return pl.pallas_call(
        functools.partial(widen_body, len(rows), len(chunks)),
        grid=(1,),
        in_specs=[SMEM] + [ANY] * (len(rows) + len(chunks)),
        out_specs=[whole(shape)] * 2,
        out_shape=[out] * 2,
        scratch_shapes=[
            pltpu.VMEM((span * len(rows), width), bf16),
            pltpu.VMEM((width, chunks[0].shape[1]), bf16),
            pltpu.SemaphoreType.DMA((len(chunks) + len(rows),)),
        ],
        compiler_params=params(32),
        name="widen",
    )(place, *rows, *chunks)


def narrow_body(count, *refs):
    hidden = refs[:2]
    chunks = refs[2 : 2 + count]
    outs = refs[2 + count : 4 + count]
    weight, sems = refs[4 + count :]
    copies = []
    start = 0
    for k, chunk in enumerate(chunks):
        copy = pltpu.make_async_copy(
            chunk, weight.at[pl.ds(start, chunk.shape[0]), :], sems.at[k]
        )
        copy.start()
        copies.append(copy)
        start += chunk.shape[0]
    for copy in copies:
        copy.wait()
    turned = weight[...].T
    for side in range(2):
        outs[side][...] = jnp.dot(
            hidden[side][...], turned, preferred_element_type=f32
        ).astype(bf16)


def narrow_call(own, other, chunks):
    columns = sum(c.shape[0] for c in chunks)
    out = jax.ShapeDtypeStruct((own.shape[0], columns), bf16)
    return pl.pallas_call(
        functools.partial(narrow_body, len(chunks)),
        grid=(1,),
        in_specs=[whole(own.shape)] * 2 + [ANY] * len(chunks),
        out_specs=[whole(out.shape)] * 2,
        out_shape=[out, out],
        scratch_shapes=[
            pltpu.VMEM((columns, chunks[0].shape[1]), bf16),
            pltpu.SemaphoreType.DMA((len(chunks),)),
        ],
        compiler_params=params(40),
        name="narrow",
    )(own, other, *chunks)


def last_body(groups, block, *refs):
    where_ref, stream_ref = refs[:2]
    near = refs[2 : 2 + groups]
    far = refs[2 + groups : 2 + 2 * groups]
    fac_ref, final_ref, out_ref, blocks, total = refs[2 + 2 * groups :]
    width = stream_ref.shape[1]
    k = 0
    for a, b in zip(near, far):
        x = a[...].astype(f32) + b[...].astype(f32)
        for low in range(0, x.shape[1], block):
            blocks[k] = x[:, low : low + block]
            k += 1
    for j in range(width // block):
        total[:, j * block : (j + 1) * block] = blocks[where_ref[j]]
    stream = stream_ref[...] + fac_ref[0, 1:2, :] * total[...]
    out_ref[...] = modulate(stream, final_ref[0, 0:1, :], final_ref[0, 1:2, :]).astype(bf16)


def last_call(images, where, stream, near, far, factors, final, block):
    rows, width = stream.shape
    span = rows // images
    return pl.pallas_call(
        functools.partial(last_body, len(near), block),
        grid=(images,),
        in_specs=[SMEM, pl.BlockSpec((span, width), lambda i: (i, 0))]
        + [pl.BlockSpec((span, x.shape[1]), lambda i: (i, 0)) for x in near + far]
        + [
            pl.BlockSpec((1,) + factors.shape[1:], lambda i: (i, 0, 0)),
            pl.BlockSpec((1,) + final.shape[1:], lambda i: (i, 0, 0)),
        ],
        out_specs=pl.BlockSpec((span, width), lambda i: (i, 0)),
        out_shape=jax.ShapeDtypeStruct((rows, width), bf16),
        scratch_shapes=[
            pltpu.VMEM((width // block, span, block), f32),
            pltpu.VMEM((span, width), f32),
        ],
        compiler_params=params(24),
        name="last",
    )(where, stream, *near, *far, factors, final)


def logit_body(half_ref, x_ref, w_ref, *rest):
    out_ref = rest[-1]
    out_ref[...] = (
        jnp.dot(x_ref[...], w_ref[...], preferred_element_type=f32)
        .astype(bf16)
        .reshape(out_ref.shape)
    )


def logit_call(images, half, x, weight, before):
    rows = x.shape[0]
    span = rows // images
    width, vocab = weight.shape
    step = 256 if vocab % 256 == 0 else vocab
    extra = [] if before is None else [before]
    return pl.pallas_call(
        logit_body,
        grid_spec=pltpu.PrefetchScalarGridSpec(
            num_scalar_prefetch=1,
            grid=(vocab // step,),
            in_specs=[
                pl.BlockSpec((rows, width), lambda n, h: (0, 0)),
                pl.BlockSpec((width, step), lambda n, h: (0, n)),
            ]
            + [ANY] * len(extra),
            out_specs=pl.BlockSpec((images, span, step), lambda n, h: (0, h[0], n)),
        ),
        out_shape=jax.ShapeDtypeStruct((images, 2 * span, vocab), bf16),
        input_output_aliases={} if before is None else {3: 0},
        compiler_params=params(24),
        name="logit",
    )(half, x, weight, *extra)


def ring_order(mesh):
    count = mesh.shape["dp"]
    axis = mesh.axis_names.index("dp")
    devices = np.moveaxis(np.asarray(mesh.devices), axis, 0).reshape(count, -1)[:, 0]
    spots = [tuple(d.coords) for d in devices]
    ys = sorted({s[1] for s in spots})
    if len(set(spots)) != count or len(ys) != 2:
        return list(range(count))
    up = sorted((s[2], k) for k, s in enumerate(spots) if s[1] == ys[0])
    down = sorted(((s[2], k) for k, s in enumerate(spots) if s[1] == ys[1]), reverse=True)
    return [k for _, k in up + down]


def build(mesh):
    n_dp = mesh.shape["dp"]
    n_tensor = mesh.shape["tensor"]
    order = ring_order(mesh)
    spot = [order.index(k) for k in range(n_dp)]
    after = {order[k]: order[(k + 1) % n_dp] for k in range(n_dp)}

    def pairs(move):
        out = []
        for d in range(n_dp):
            for t in range(n_tensor):
                e, u = move(d, t)
                out.append((d * n_tensor + t, e * n_tensor + u))
        return out

    ring = [
        pairs(lambda d, t: (after[d], t)),
        [(b, a) for a, b in pairs(lambda d, t: (after[d], t))],
    ]
    twin = pairs(lambda d, t: (d, t ^ 1))

    def swap(x):
        return lax.ppermute(x, AXES, twin)

    def across(x):
        total = None
        for r in range(1, n_tensor // 2):
            y = lax.ppermute(x, AXES, pairs(lambda d, t: (d, (t + 2 * r) % n_tensor)))
            total = y if total is None else total + y
        return total

    def gather(shard):
        rows = shard.shape[0]
        if n_dp % 2 or rows % 32:
            return [(lax.all_gather(shard, "dp", axis=0, tiled=True), None, 0)]
        part = rows // 2
        found = [(shard, 0, 0)]
        for p in range(2):
            for way in range(2):
                x = shard[p * part : (p + 1) * part]
                for s in range(1, n_dp // 2 + 1):
                    if s == n_dp // 2 and way != p:
                        break
                    x = lax.ppermute(x, AXES, ring[way])
                    found.append((x, -s if way == 0 else s, p * part))
        return found

    def local(
        tokens,
        book,
        base,
        lift,
        loc,
        factors,
        sharp,
        w_qkv,
        w_out,
        w_up,
        w_down,
        old_k,
        old_v,
        final,
        w_vocab,
    ):
        images = tokens.shape[0]
        heads = sharp.shape[1]
        size = old_k.shape[3] // heads
        shard_rows = w_qkv.shape[1]
        width = loc.shape[1]
        factors = factors[0]
        dp = lax.axis_index("dp")
        half = (lax.axis_index("tensor") % 2).astype(jnp.int32)
        own_half = half.reshape(1)
        other_half = (1 - half).reshape(1)
        here = jnp.asarray(spot, jnp.int32)[dp]
        table = jnp.asarray(order, jnp.int32)

        def sources(found):
            if found[0][1] is None:
                return jnp.zeros((1,), jnp.int32)
            away = jnp.asarray([f[1] for f in found], jnp.int32)
            inner = jnp.asarray([f[2] for f in found], jnp.int32)
            return table[(here + away) % n_dp] * shard_rows + inner

        front = jnp.concatenate(
            [w_qkv[0].reshape(shard_rows, -1), w_out[0].T], axis=1
        )
        front = gather(front)
        up = gather(w_up[0])
        down = gather(w_down[0].T)
        place = sources(front)

        up_matrix = interp_matrix(math.isqrt(loc.shape[0]), math.isqrt(tokens.shape[1]))
        kron = jnp.asarray(np.kron(up_matrix, up_matrix))
        canvas = canvas_call(tokens, book.T, kron, base)

        streams, normed = [], []
        for i in range(images):
            x, s = enter_call(i, own_half, canvas, lift, loc, factors)
            normed.append(x)
            streams.append(s)

        own, other = [], []
        stream = None
        for i in range(images):
            keep, send = attend_call(
                i, heads, size, sharp, place, normed[i], old_k, old_v, [f[0] for f in front]
            )
            near = keep + swap(send)
            far = across(near)
            stream, x = mid_call(i, images, streams[i], near, far, factors, stream)
            own.append(x)
            other.append(swap(x))

        up_place = sources(up)
        hidden = widen_call(up_place, own + other, [f[0] for f in up])

        if down[0][1] is None:
            block = width
            groups = [[0]]
            by_distance = {0: [down[0][0]]}
            spread = [0]
            where = jnp.zeros((1,), jnp.int32)
        else:
            block = shard_rows
            half_ring = n_dp // 2
            by_distance = {}
            for x, away, inner in down:
                key = half_ring if abs(away) == half_ring else away
                by_distance.setdefault(key, []).append((inner, x))
            by_distance = {
                k: [x for _, x in sorted(v, key=lambda e: e[0])] for k, v in by_distance.items()
            }
            groups = [[0, -1, 1]] + [[-s, s] for s in range(2, half_ring)] + [[half_ring]]
            spread = [a for g in groups for a in g]
            turn = [0] * n_dp
            for k, a in enumerate(spread):
                turn[a % n_dp] = k
            dest = jnp.asarray(spot, jnp.int32)
            where = jnp.asarray(turn, jnp.int32)[(dest - here) % n_dp]
        near, far = [], []
        for members in groups:
            chunks = [x for a in members for x in by_distance[a]]
            keep, send = narrow_call(hidden[0], hidden[1], chunks)
            x = keep + swap(send)
            near.append(x)
            far.append(across(x))

        mine = last_call(images, where, stream, near, far, factors, final, block)
        theirs = swap(mine)
        logits = logit_call(images, own_half, mine, w_vocab, None)
        logits = logit_call(images, other_half, theirs, w_vocab, logits)
        return logits, canvas

    return local


def solution(mesh):
    placed = (
        P("dp", None),
        P(),
        P("dp", None, None),
        P(),
        P(),
        P(None, "dp", None, None),
        P(None, "tensor"),
        P(None, "dp", None, "tensor"),
        P(None, "tensor", "dp"),
        P(None, "dp", "tensor"),
        P(None, "tensor", "dp"),
        P(None, "dp", None, "tensor"),
        P(None, "dp", None, "tensor"),
        P("dp", None, None),
        P(None, "tensor"),
    )
    return jax.shard_map(
        build(mesh),
        mesh=mesh,
        in_specs=placed,
        out_specs=(P("dp", None, "tensor"), P("dp", None, None)),
        check_vma=False,
    )
```

```python
import functools
import math

import jax
import jax.numpy as jnp
import numpy as np
from jax import lax
from jax.experimental import pallas as pl
from jax.experimental.pallas import tpu as pltpu
from jax.sharding import PartitionSpec as P


norm_floor = 0.1
highest = lax.Precision.HIGHEST
f32 = jnp.float32
bf16 = jnp.bfloat16
ANY = pl.BlockSpec(memory_space=pl.ANY)
SMEM = pl.BlockSpec(memory_space=pltpu.SMEM)
AXES = ("dp", "tensor")


def interp_matrix(grid_side, prev_side):
    out = np.zeros((grid_side, prev_side), np.float32)
    for a in range(grid_side):
        top = max((2 * a + 1) * prev_side - grid_side, 0)
        low = top // (2 * grid_side)
        frac = (top % (2 * grid_side)) / (2.0 * grid_side)
        out[a, low] += 1.0 - frac
        out[a, min(low + 1, prev_side - 1)] += frac
    return out


def whole(shape):
    return pl.BlockSpec(shape, lambda *_: (0,) * len(shape))


def params(mib):
    return pltpu.CompilerParams(vmem_limit_bytes=mib * 1024 * 1024)


def split3(x):
    hi = x.astype(bf16)
    rest = x - hi.astype(f32)
    mid = rest.astype(bf16)
    low = (rest - mid.astype(f32)).astype(bf16)
    return hi, mid, low


NT = (((1,), (1,)), ((), ()))


def canvas_body(tok_ref, book_ref, kron_ref, base_ref, out_ref):
    rows = book_ref.shape[0]
    entries = book_ref.shape[1]
    tok = tok_ref[0]
    ids = lax.broadcasted_iota(jnp.int32, (entries, tok.shape[1]), 0)
    onehot = jnp.where(ids == tok, 1.0, 0.0).astype(bf16)
    parts = jnp.concatenate(split3(book_ref[...]), axis=0)
    picked = jnp.dot(parts, onehot, preferred_element_type=f32)
    picked = picked[:rows] + picked[rows : 2 * rows] + picked[2 * rows :]
    out_ref[0] = base_ref[0] + jnp.dot(
        picked, kron_ref[...], precision=highest, preferred_element_type=f32
    )


def canvas_call(tokens, book, kron, base):
    images, count = tokens.shape
    block = pl.BlockSpec((1,) + base.shape[1:], lambda i: (i, 0, 0))
    return pl.pallas_call(
        canvas_body,
        grid=(images,),
        in_specs=[
            pl.BlockSpec((1, 1, count), lambda i: (i, 0, 0)),
            whole(book.shape),
            whole(kron.shape),
            block,
        ],
        out_specs=block,
        out_shape=jax.ShapeDtypeStruct(base.shape, f32),
        compiler_params=params(24),
        name="canvas",
    )(tokens.reshape(images, 1, count), book, kron, base)


def modulate(stream, scale_vec, shift_vec):
    center = stream - jnp.mean(stream, axis=-1, keepdims=True)
    variance = jnp.mean(center * center, axis=-1, keepdims=True)
    return center * lax.rsqrt(variance + norm_floor) * (1.0 + scale_vec) + shift_vec


def enter_body(info_ref, canvas_ref, lift_ref, loc_ref, fac_ref, normed_ref, stream_ref):
    span = stream_ref.shape[0]
    for k in range(2):
        start = pl.multiple_of(info_ref[k] * span, span)
        stream = (
            jnp.dot(
                canvas_ref[0, :, pl.ds(start, span)].T,
                lift_ref[...],
                precision=highest,
                preferred_element_type=f32,
            )
            + loc_ref[pl.ds(start, span), :]
        )
        if k == 0:
            stream_ref[...] = stream
        normed_ref[pl.ds(k * span, span), :] = modulate(
            stream, fac_ref[0, 2:3, :], fac_ref[0, 4:5, :]
        ).astype(bf16)


def enter_call(info, first, batch, canvas, lift, loc, factors):
    tokens, width = loc.shape
    return pl.pallas_call(
        enter_body,
        grid=(batch,),
        in_specs=[
            SMEM,
            pl.BlockSpec((1,) + canvas.shape[1:], lambda i: (first + i, 0, 0)),
            whole(lift.shape),
            whole(loc.shape),
            pl.BlockSpec((1,) + factors.shape[1:], lambda i: (first + i, 0, 0)),
        ],
        out_specs=[
            pl.BlockSpec((tokens, width), lambda i: (i, 0)),
            pl.BlockSpec((tokens // 2, width), lambda i: (i, 0)),
        ],
        out_shape=[
            jax.ShapeDtypeStruct((batch * tokens, width), bf16),
            jax.ShapeDtypeStruct((batch * tokens // 2, width), f32),
        ],
        compiler_params=params(24),
        name="enter",
    )(info, canvas, lift, loc, factors)


def head_windows(heads, size):
    total = heads * size
    spans = []
    for h in range(heads):
        low = (h * size) // 128 * 128
        high = min(-(-((h + 1) * size) // 128) * 128, total)
        spans.append((low, high))
    return spans


def head_scale(x, heads, size, extra):
    lane = lax.broadcasted_iota(jnp.int32, (1, x.shape[1]), 1)
    square = x * x
    scale = None
    for h, (low, high) in enumerate(head_windows(heads, size)):
        inside = (lane[:, low:high] >= h * size) & (lane[:, low:high] < (h + 1) * size)
        total = jnp.sum(jnp.where(inside, square[:, low:high], 0.0), axis=1, keepdims=True)
        factor = lax.rsqrt(total + 1.0)
        if extra is not None:
            factor = factor * extra(h)
        if scale is None:
            scale = jnp.broadcast_to(factor, x.shape)
        else:
            scale = jnp.where(lane >= h * size, factor, scale)
    return (x * scale).astype(bf16)


def attend_body(heads, size, count, *refs):
    info_ref, sharp_ref, normed_ref, oldk_ref, oldv_ref = refs[:5]
    chunks = refs[5 : 5 + count]
    keep_ref, send_ref, weight, sems = refs[5 + count :]
    width = heads * size
    copies = []
    for k, chunk in enumerate(chunks):
        start = pl.multiple_of(info_ref[2 + k], 16)
        copies.append(
            pltpu.make_async_copy(
                chunk, weight.at[pl.ds(start, chunk.shape[0]), :], sems.at[k]
            )
        )

    @pl.when(pl.program_id(0) == 0)
    def _():
        for copy in copies:
            copy.start()

    key_old = head_scale(oldk_ref[0, 0].astype(f32), heads, size, None)
    value_old = oldv_ref[0, 0]

    @pl.when(pl.program_id(0) == 0)
    def _():
        for copy in copies:
            copy.wait()

    normed = normed_ref[...]
    part = [
        jnp.dot(normed, weight[:, k * width : (k + 1) * width], preferred_element_type=f32)
        for k in range(3)
    ]
    query = head_scale(part[0], heads, size, lambda h: sharp_ref[0, h])
    key_new = head_scale(part[1], heads, size, None)
    value_new = part[2].astype(bf16)
    lane = lax.broadcasted_iota(jnp.int32, (1, width), 1)
    rows = normed.shape[0]
    pieces = [jnp.zeros((rows, 128), f32) for _ in range(-(-width // 128))]
    for h, (low, high) in enumerate(head_windows(heads, size)):
        inside = (lane[:, low:high] >= h * size) & (lane[:, low:high] < (h + 1) * size)
        q = jnp.where(inside, query[:, low:high].astype(f32), 0.0).astype(bf16)
        s_old = lax.dot_general(q, key_old[:, low:high], NT, preferred_element_type=f32)
        s_new = lax.dot_general(q, key_new[:, low:high], NT, preferred_element_type=f32)
        top = jnp.maximum(
            jnp.max(s_old, axis=1, keepdims=True), jnp.max(s_new, axis=1, keepdims=True)
        )
        e_old = jnp.exp(s_old - top)
        e_new = jnp.exp(s_new - top)
        total = jnp.sum(e_old, axis=1, keepdims=True) + jnp.sum(e_new, axis=1, keepdims=True)
        out = jnp.dot(e_old.astype(bf16), value_old[:, low:high], preferred_element_type=f32)
        out = out + jnp.dot(
            e_new.astype(bf16), value_new[:, low:high], preferred_element_type=f32
        )
        out = jnp.where(inside, out * (1.0 / total), 0.0)
        for t in range(low // 128, -(-high // 128)):
            at = t * 128 - low
            pieces[t] = pieces[t] + out[:, at : at + 128]
    attended = jnp.concatenate(pieces, axis=1)[:, :width].astype(bf16)
    mixed = lax.dot_general(
        attended, weight[:, 3 * width :], NT, preferred_element_type=f32
    ).astype(bf16)
    keep_ref[...] = mixed[: rows // 2]
    send_ref[...] = mixed[rows // 2 :]


def attend_call(info, first, batch, heads, size, sharp, normed, old_k, old_v, chunks):
    width = normed.shape[1]
    rows = normed.shape[0] // batch
    cache = pl.BlockSpec((1, 1) + old_k.shape[2:], lambda i: (0, first + i, 0, 0))
    out = jax.ShapeDtypeStruct((normed.shape[0] // 2, width), bf16)
    return pl.pallas_call(
        functools.partial(attend_body, heads, size, len(chunks)),
        grid=(batch,),
        in_specs=[SMEM, SMEM, pl.BlockSpec((rows, width), lambda i: (i, 0)), cache, cache]
        + [ANY] * len(chunks),
        out_specs=[pl.BlockSpec((rows // 2, width), lambda i: (i, 0))] * 2,
        out_shape=[out, out],
        scratch_shapes=[
            pltpu.VMEM((width, chunks[0].shape[1]), bf16),
            pltpu.SemaphoreType.DMA((len(chunks),)),
        ],
        compiler_params=params(32),
        name="attend",
    )(info, sharp, normed, old_k, old_v, *chunks)


def mid_body(stream_ref, near_ref, far_ref, fac_ref, *rest):
    out_ref, normed_ref = rest[-2:]
    mixed = near_ref[...].astype(f32) + far_ref[...].astype(f32)
    stream = stream_ref[...] + fac_ref[0, 0:1, :] * mixed
    out_ref[...] = stream
    normed_ref[...] = modulate(stream, fac_ref[0, 3:4, :], fac_ref[0, 5:6, :]).astype(bf16)


def mid_call(first, batch, images, stream, near, far, factors, before):
    rows, width = stream.shape
    steps = 2
    span = rows // batch // steps
    spec = pl.BlockSpec((span, width), lambda k: (k, 0))
    extra = [] if before is None else [before]
    return pl.pallas_call(
        mid_body,
        grid=(batch * steps,),
        in_specs=[
            spec,
            spec,
            spec,
            pl.BlockSpec((1,) + factors.shape[1:], lambda k: (first + k // steps, 0, 0)),
        ]
        + [ANY] * len(extra),
        out_specs=[
            pl.BlockSpec((span, width), lambda k: (first * steps + k, 0)),
            spec,
        ],
        out_shape=[
            jax.ShapeDtypeStruct((images * rows // batch, width), f32),
            jax.ShapeDtypeStruct(stream.shape, bf16),
        ],
        input_output_aliases={4: 0} if extra else {},
        compiler_params=params(16),
        name="mid",
    )(stream, near, far, factors, *extra)


def widen_body(pieces, count, *refs):
    info_ref = refs[0]
    rows_refs = refs[1 : 1 + pieces]
    chunks = refs[1 + pieces : 1 + pieces + count]
    outs = refs[1 + pieces + count : 3 + pieces + count]
    source, weight, sems = refs[3 + pieces + count :]
    span = rows_refs[0].shape[0]
    copies = []
    for k, chunk in enumerate(chunks):
        start = pl.multiple_of(info_ref[2 + k], 16)
        copies.append(
            pltpu.make_async_copy(
                chunk, weight.at[pl.ds(start, chunk.shape[0]), :], sems.at[k]
            )
        )
    for k, piece in enumerate(rows_refs):
        copies.append(
            pltpu.make_async_copy(
                piece, source.at[k * span : (k + 1) * span, :], sems.at[count + k]
            )
        )
    for copy in copies:
        copy.start()
    for copy in copies:
        copy.wait()
    step = 512 if weight.shape[1] % 512 == 0 else weight.shape[1]
    half = source.shape[0] // 2

    @pl.loop(0, weight.shape[1] // step)
    def _(n):
        low = pl.multiple_of(n * step, step)
        for k in range(2):
            u = jnp.dot(
                source[k * half : (k + 1) * half, :],
                weight[:, pl.ds(low, step)],
                preferred_element_type=f32,
            )
            outs[k][:, pl.ds(low, step)] = (
                0.5 * u * (1.0 + jnp.tanh(math.sqrt(2.0 / math.pi) * (u + 0.044715 * (u * u * u))))
            ).astype(bf16)


def widen_call(info, rows, chunks):
    span, width = rows[0].shape
    shape = (span * len(rows) // 2, chunks[0].shape[1])
    out = jax.ShapeDtypeStruct(shape, bf16)
    return pl.pallas_call(
        functools.partial(widen_body, len(rows), len(chunks)),
        grid=(1,),
        in_specs=[SMEM] + [ANY] * (len(rows) + len(chunks)),
        out_specs=[whole(shape)] * 2,
        out_shape=[out] * 2,
        scratch_shapes=[
            pltpu.VMEM((span * len(rows), width), bf16),
            pltpu.VMEM((width, chunks[0].shape[1]), bf16),
            pltpu.SemaphoreType.DMA((len(chunks) + len(rows),)),
        ],
        compiler_params=params(32),
        name="widen",
    )(info, *rows, *chunks)


def narrow_body(count, *refs):
    hidden = refs[:2]
    chunks = refs[2 : 2 + count]
    outs = refs[2 + count : 4 + count]
    weight, sems = refs[4 + count :]
    copies = []
    start = 0
    for k, chunk in enumerate(chunks):
        copy = pltpu.make_async_copy(
            chunk, weight.at[pl.ds(start, chunk.shape[0]), :], sems.at[k]
        )
        copy.start()
        copies.append(copy)
        start += chunk.shape[0]
    for copy in copies:
        copy.wait()
    turned = weight[...].T
    columns = turned.shape[1]
    for side in range(2):
        part = jnp.dot(hidden[side][...], turned, preferred_element_type=f32).astype(bf16)
        for k in range(outs[side].shape[1] // columns):
            span = outs[side].shape[0]
            outs[side][:, k * columns : (k + 1) * columns] = part[k * span : (k + 1) * span]


def narrow_call(own, other, chunks, fold):
    columns = sum(c.shape[0] for c in chunks)
    out = jax.ShapeDtypeStruct((own.shape[0] // fold, columns * fold), bf16)
    return pl.pallas_call(
        functools.partial(narrow_body, len(chunks)),
        grid=(1,),
        in_specs=[whole(own.shape)] * 2 + [ANY] * len(chunks),
        out_specs=[whole(out.shape)] * 2,
        out_shape=[out, out],
        scratch_shapes=[
            pltpu.VMEM((columns, chunks[0].shape[1]), bf16),
            pltpu.SemaphoreType.DMA((len(chunks),)),
        ],
        compiler_params=params(40),
        name="narrow",
    )(own, other, *chunks)


def last_body(folds, layout, block, first, *refs):
    groups = len(folds)
    info_ref, stream_ref = refs[:2]
    near = refs[2 : 2 + groups]
    far = refs[2 + groups : 2 + 2 * groups]
    fac_ref, final_ref, out_ref, blocks, total = refs[2 + 2 * groups :]
    width = stream_ref.shape[1]
    upper = pl.program_id(0) >= pl.num_programs(0) // 2
    for fold, parts, a, b in zip(folds, layout, near, far):
        x = a[...].astype(f32) + b[...].astype(f32)
        if fold == 2:
            x = jnp.where(upper, x[:, x.shape[1] // 2 :], x[:, : x.shape[1] // 2])
        for k, inner, low, size in parts:
            blocks[k, :, inner : inner + size] = x[:, low : low + size]
    for j in range(width // block):
        total[:, j * block : (j + 1) * block] = blocks[info_ref[first + j]]
    stream = stream_ref[...] + fac_ref[0, 1:2, :] * total[...]
    out_ref[...] = modulate(stream, final_ref[0, 0:1, :], final_ref[0, 1:2, :]).astype(bf16)


def last_call(
    images, info, first, stream, near, far, folds, layout, factors, final, block
):
    rows, width = stream.shape
    span = rows // images
    return pl.pallas_call(
        functools.partial(last_body, folds, layout, block, first),
        grid=(images,),
        in_specs=[SMEM, pl.BlockSpec((span, width), lambda i: (i, 0))]
        + [
            pl.BlockSpec((span, x.shape[1]), lambda i, m=images // fold: (i % m, 0))
            for x, fold in zip(near + far, folds + folds)
        ]
        + [
            pl.BlockSpec((1,) + factors.shape[1:], lambda i: (i, 0, 0)),
            pl.BlockSpec((1,) + final.shape[1:], lambda i: (i, 0, 0)),
        ],
        out_specs=pl.BlockSpec((span, width), lambda i: (i, 0)),
        out_shape=jax.ShapeDtypeStruct((rows, width), bf16),
        scratch_shapes=[
            pltpu.VMEM((width // block, span, block), f32),
            pltpu.VMEM((span, width), f32),
        ],
        compiler_params=params(24),
        name="last",
    )(info, stream, *near, *far, factors, final)


def fetch_body(w_ref, out_ref, sem):
    copy = pltpu.make_async_copy(w_ref, out_ref, sem)
    copy.start()
    copy.wait()


def fetch_call(weight):
    return pl.pallas_call(
        fetch_body,
        in_specs=[pl.BlockSpec(memory_space=pltpu.HBM)],
        out_specs=pl.BlockSpec(memory_space=pltpu.VMEM),
        out_shape=pltpu.VMEM(weight.shape, weight.dtype),
        scratch_shapes=[pltpu.SemaphoreType.DMA],
        compiler_params=params(8),
        name="fetch",
    )(pltpu.with_memory_space_constraint(weight, pltpu.HBM))


def logit_body(info_ref, x_ref, w_ref, *rest):
    out_ref = rest[-1]
    out_ref[...] = (
        jnp.dot(x_ref[...], w_ref[...], preferred_element_type=f32)
        .astype(bf16)
        .reshape(out_ref.shape)
    )


def logit_call(images, side, info, x, weight, before):
    rows = x.shape[0]
    span = rows // images
    width, vocab = weight.shape
    step = 512 if vocab % 512 == 0 else vocab
    extra = [] if before is None else [before]
    return pl.pallas_call(
        logit_body,
        grid_spec=pltpu.PrefetchScalarGridSpec(
            num_scalar_prefetch=1,
            grid=(vocab // step,),
            in_specs=[
                whole((rows, width)),
                pl.BlockSpec((width, step), lambda n, t: (0, n)),
            ]
            + [ANY] * len(extra),
            out_specs=pl.BlockSpec((images, span, step), lambda n, t: (0, t[side], n)),
        ),
        out_shape=jax.ShapeDtypeStruct((images, 2 * span, vocab), bf16),
        input_output_aliases={} if before is None else {3: 0},
        compiler_params=params(24),
        name="logit",
    )(info, x, weight, *extra)


def ring_order(mesh):
    count = mesh.shape["dp"]
    axis = mesh.axis_names.index("dp")
    devices = np.moveaxis(np.asarray(mesh.devices), axis, 0).reshape(count, -1)[:, 0]
    spots = [tuple(d.coords) for d in devices]
    ys = sorted({s[1] for s in spots})
    if len(set(spots)) != count or len(ys) != 2:
        return list(range(count))
    up = sorted((s[2], k) for k, s in enumerate(spots) if s[1] == ys[0])
    down = sorted(((s[2], k) for k, s in enumerate(spots) if s[1] == ys[1]), reverse=True)
    return [k for _, k in up + down]


def build(mesh):
    n_dp = mesh.shape["dp"]
    n_tensor = mesh.shape["tensor"]
    order = ring_order(mesh)
    spot = [order.index(k) for k in range(n_dp)]
    after = {order[k]: order[(k + 1) % n_dp] for k in range(n_dp)}

    def pairs(move):
        out = []
        for d in range(n_dp):
            for t in range(n_tensor):
                e, u = move(d, t)
                out.append((d * n_tensor + t, e * n_tensor + u))
        return out

    ring = [
        pairs(lambda d, t: (after[d], t)),
        [(b, a) for a, b in pairs(lambda d, t: (after[d], t))],
    ]
    twin = pairs(lambda d, t: (d, t ^ 1))

    def swap(x):
        return lax.ppermute(x, AXES, twin)

    def across(x):
        total = None
        for r in range(1, n_tensor // 2):
            y = lax.ppermute(x, AXES, pairs(lambda d, t: (d, (t + 2 * r) % n_tensor)))
            total = y if total is None else total + y
        return total

    def gather(shard):
        rows = shard.shape[0]
        if n_dp % 2 or rows % 32:
            return [(lax.all_gather(shard, "dp", axis=0, tiled=True), None, 0)]
        part = rows // 2
        found = [(shard, 0, 0)]
        for p in range(2):
            for way in range(2):
                x = shard[p * part : (p + 1) * part]
                for s in range(1, n_dp // 2 + 1):
                    if s == n_dp // 2 and way != p:
                        break
                    x = lax.ppermute(x, AXES, ring[way])
                    found.append((x, -s if way == 0 else s, p * part))
        return found

    def local(
        tokens,
        book,
        base,
        lift,
        loc,
        factors,
        sharp,
        w_qkv,
        w_out,
        w_up,
        w_down,
        old_k,
        old_v,
        final,
        w_vocab,
    ):
        images = tokens.shape[0]
        heads = sharp.shape[1]
        size = old_k.shape[3] // heads
        shard_rows = w_qkv.shape[1]
        width = loc.shape[1]
        factors = factors[0]
        front = jnp.concatenate(
            [w_qkv[0].reshape(shard_rows, -1), w_out[0].T], axis=1
        )
        front = gather(front)
        up = gather(w_up[0])
        down = gather(w_down[0].T)

        half_ring = n_dp // 2
        ringed = down[0][1] is not None
        block = shard_rows if ringed else width
        part = shard_rows // 2
        by_name = {(away, inner): x for x, away, inner in down}
        groups = [[(down[0][1], 0)]]
        if ringed:
            sets = [
                [[(-s, 0), (s, part)], [(-s, part), (s, 0)]] for s in range(1, half_ring)
            ]
            for a, b in sets[:-1]:
                groups.append(sorted(a + b))
            groups += [sets[-1][0], sets[-1][1], [(-half_ring, 0), (half_ring, part)]]
        turn = {}
        layout = []
        for g in groups:
            layout.append([])
            low = 0
            for away, inner in g:
                k = turn.setdefault((away or 0) % n_dp, len(turn))
                count = by_name[away, inner].shape[0]
                before = layout[-1][-1] if layout[-1] else (None, 0, 0, 0)
                if before[0] == k and before[1] + before[3] == inner:
                    layout[-1][-1] = (k, before[1], before[2], before[3] + count)
                else:
                    layout[-1].append((k, inner, low, count))
                low += count

        rows = []
        for d in range(n_dp):
            place = [
                0 if away is None else order[(spot[d] + away) % n_dp] * shard_rows + inner
                for _, away, inner in front
            ]
            where = [
                turn[(spot[j] - spot[d]) % n_dp] if ringed else 0
                for j in range(width // block)
            ]
            rows += [[half, 1 - half] + place + where for half in range(2)]
        pick = lax.axis_index("dp") * 2 + lax.axis_index("tensor") % 2
        info = lax.dynamic_slice(
            jnp.asarray(np.asarray(rows, np.int32)), (pick, 0), (1, len(rows[0]))
        ).reshape(-1)
        first_block = 2 + len(front)

        up_matrix = interp_matrix(math.isqrt(loc.shape[0]), math.isqrt(tokens.shape[1]))
        kron = jnp.asarray(np.ascontiguousarray(np.kron(up_matrix, up_matrix).T))
        canvas = canvas_call(tokens, book.T, kron, base.swapaxes(1, 2))

        batch = 2 if images % 2 == 0 else 1
        starts = range(0, images, batch)
        entered = []
        for first in starts:
            entered.append(enter_call(info, first, batch, canvas, lift, loc, factors))

        own, other = [], []
        stream = None
        for p, first in enumerate(starts):
            keep, send = attend_call(
                info,
                first,
                batch,
                heads,
                size,
                sharp,
                entered[p][0],
                old_k,
                old_v,
                [f[0] for f in front],
            )
            near = keep + swap(send)
            far = across(near)
            stream, x = mid_call(first, batch, images, entered[p][1], near, far, factors, stream)
            own.append(x)
            other.append(swap(x))

        hidden = widen_call(info, own + other, [f[0] for f in up])

        near, far, folds = [], [], []
        for members in groups:
            chunks = [by_name[a] for a in members]
            columns = sum(c.shape[0] for c in chunks)
            folds.append(2 if images % 2 == 0 and columns % 128 else 1)
            keep, send = narrow_call(hidden[0], hidden[1], chunks, folds[-1])
            x = keep + swap(send)
            near.append(x)
            far.append(across(x))

        w_vocab = fetch_call(w_vocab)
        mine = last_call(
            images, info, first_block, stream, near, far, folds, layout, factors, final, block
        )
        theirs = swap(mine)
        logits = logit_call(images, 0, info, mine, w_vocab, None)
        logits = logit_call(images, 1, info, theirs, w_vocab, logits)
        return logits, canvas.swapaxes(1, 2)

    return local


def solution(mesh):
    placed = (
        P("dp", None),
        P(),
        P("dp", None, None),
        P(),
        P(),
        P(None, "dp", None, None),
        P(None, "tensor"),
        P(None, "dp", None, "tensor"),
        P(None, "tensor", "dp"),
        P(None, "dp", "tensor"),
        P(None, "tensor", "dp"),
        P(None, "dp", None, "tensor"),
        P(None, "dp", None, "tensor"),
        P("dp", None, None),
        P(None, "tensor"),
    )
    return jax.shard_map(
        build(mesh),
        mesh=mesh,
        in_specs=placed,
        out_specs=(P("dp", None, "tensor"), P("dp", None, None)),
        check_vma=False,
    )
```
